32 devices in a mesh: energy: 4 (over z), orb: 4 (over y, x), kpt: 2 (over core).
Axes of the slice: x: 2, y: 2, z: 4, core: 2. Of those that a mesh axis runs over, the one named last changes fastest.
Arguments:
- lesser: bfloat16 [2, 4, 16, 1, 512, 512], P(None, 'energy', 'kpt', None, None, 'orb'), may hold values from -6 to 6
- coupling: bfloat16 [2, 16, 512, 512], P(None, None, None, 'orb'), may hold values from -0.046875 to 0.046875
- transfer_map: int32 [16, 16], replicated, may hold values from 0 to 15, as said below
Outputs:
- sigma: bfloat16 [2, 4, 16, 1, 512, 512], P(None, None, 'kpt', None, 'energy', 'orb')
The draws below stay inside these ranges and needn't reach their ends.
Inputs may be any that keep to these rules, and one draw needn't show every extreme that they name: transfer_map[k, p] is the index of the momentum transfer k - p: each row and each column holds every number of 0 to 15 once.
All inputs are finite; a program needn't handle non-finite values.
Results may differ from the reference program's by a relative error of at most 0.001.
Values may be sent and summed in bfloat16 or wider, within the bound.
A program may use at most 128 MiB of HBM per device.

```python
import jax
import jax.numpy as jnp
from jax import lax

NO = 512
LAYERS = 1
K = 16
ENERGIES = 4


def draw_transfer_map(key, part):
    ranking = jax.random.permutation(jax.random.fold_in(key, 7), K).astype(jnp.int32)
    target_ids = jnp.arange(K, dtype=jnp.int32)
    shifts = (target_ids[:, None] - target_ids[None, :]) % K
    return ranking[shifts]


def shard_levels(stream_key, shape, shards, low, largest):
    def one(position, parts):
        draws = jax.random.uniform(jax.random.fold_in(jax.random.fold_in(stream_key, 6), position), (parts,), jnp.float32, low / len(shards), largest / len(shards))
        return jnp.repeat(jnp.exp(draws), shape[position] // parts).reshape((-1,) + (1,) * (len(shape) - position - 1))

    factor_of = one(*shards[0])
    for cut in shards[1:]:
        factor_of = factor_of * one(*cut)
    return factor_of


def normal_values(rng, shape, spread, bound, split=(), kind=jnp.bfloat16):
    result = jax.random.normal(rng, shape, jnp.float32) * spread
    if len(split) > 0:
        result = shard_levels(rng, shape, split, -0.22, 0.18) * result
    return jnp.clip(result, min=-bound, max=bound).astype(kind)


def setup_inputs(seed: int = 0) -> dict:
    key_of = jax.random.split(jax.random.key(seed), 4)
    return {
        "lesser": normal_values(key_of[0], (2, ENERGIES, K, LAYERS, NO, NO), 1.0, 6.0, ((1, 4), (2, 2), (5, 4))),
        "coupling": normal_values(key_of[1], (2, K, NO, NO), (2 * NO * K) ** -0.5, 0.046875, ((3, 4),)),
        "transfer_map": draw_transfer_map(jax.random.fold_in(key_of[3], 71), 0),
    }


def reference(lesser, coupling, transfer_map):
    real_green = lesser[0].astype(jnp.float32)
    imag_green = lesser[1].astype(jnp.float32)

    def per_target(target):
        selected = jnp.take(coupling, transfer_map[target], axis=1).astype(jnp.float32)
        real_out = jnp.einsum("eplrm,pmj->elrj", real_green, selected[0]) - jnp.einsum("eplrm,pmj->elrj", imag_green, selected[1])
        imag_out = jnp.einsum("eplrm,pmj->elrj", real_green, selected[1]) + jnp.einsum("eplrm,pmj->elrj", imag_green, selected[0])
        return jnp.stack([real_out, imag_out]).astype(jnp.bfloat16)

    stacked = lax.map(per_target, jnp.arange(K, dtype=jnp.int32))
    return jnp.transpose(stacked, (1, 2, 0, 3, 4, 5))
```

```python
import functools

import jax
import jax.numpy as jnp
from jax import lax
from jax.experimental import pallas as pl
from jax.experimental.pallas import tpu as pltpu
from jax.sharding import PartitionSpec as P

MESH = pl.DeviceIdType.MESH
DA, DB, P0, PX, PY, PD = range(6)
RELAY, DIAG, MULTIPLY = 2, 4, 5


def complex_terms(green, selected):
    real_out = jnp.einsum(
        "prm,tpmj->trj", green[0], selected[0], preferred_element_type=jnp.float32
    ) - jnp.einsum("prm,tpmj->trj", green[1], selected[1], preferred_element_type=jnp.float32)
    imag_out = jnp.einsum(
        "prm,tpmj->trj", green[0], selected[1], preferred_element_type=jnp.float32
    ) + jnp.einsum("prm,tpmj->trj", green[1], selected[0], preferred_element_type=jnp.float32)
    return (real_out, imag_out)


def per_device_general(lesser, coupling, transfer_map):
    regrouped = lax.all_to_all(lesser, "energy", split_axis=4, concat_axis=1, tiled=True)
    gathered = lax.all_gather(regrouped, "orb", axis=5, tiled=True)
    energies = gathered.shape[1]
    local_points = gathered.shape[2]
    layers = gathered.shape[3]
    tile = gathered.shape[4]
    width = gathered.shape[5]
    out_cols = coupling.shape[3]
    row_count = energies * layers * tile
    first_point = lax.axis_index("kpt") * local_points
    reordered = jnp.moveaxis(gathered, 2, 1).reshape(2, local_points, row_count, width)
    my_columns = lax.dynamic_slice_in_dim(transfer_map, first_point, local_points, 1)
    selected = jnp.take(coupling, my_columns, axis=1)
    real_out, imag_out = complex_terms(reordered, selected)
    mine = lax.psum_scatter(
        jnp.stack([real_out, imag_out], axis=1), "kpt", scatter_dimension=0, tiled=True
    )
    summed = jnp.moveaxis(mine, 1, 0)
    result = summed.astype(jnp.bfloat16).reshape(2, local_points, energies, layers, tile, out_cols)
    return jnp.moveaxis(result, 1, 2)


def kernel(nz, map_hbm, lesser, coupling, out, g, u, acc, map_ref, zsend, zrecv, osend, orecv, send, recv, local_sem, u_sem, map_sem):
    points = lesser.shape[2]
    width = lesser.shape[5]
    tile = g.shape[5]
    ticks = nz * points
    e = lax.axis_index("energy")
    o = lax.axis_index("orb")
    c = lax.axis_index("kpt")
    ox = o + 1 - 2 * lax.rem(o, 2)
    oy = lax.rem(o + 2, 4)
    od = 3 - o
    cp = 1 - c
    to_x, to_y, to_peer = {"orb": ox}, {"orb": oy}, {"kpt": cp}

    def offset(i):
        phase = lax.div(i, points)
        near = lax.div(phase + 1, 2)
        return lax.select(lax.rem(phase, 2) == 1, near, lax.rem(nz - lax.div(phase, 2), nz))

    def point(i):
        return lax.rem(i, points)

    def to_energy(d):
        return lax.rem(e + d, nz)

    def owner(i):
        return lax.rem(e + nz - offset(i), nz)

    def own_rows(s, z):
        return lesser.at[:, 0, s, 0, pl.ds(pl.multiple_of(z * tile, tile), tile), :]

    def block(k, q, i):
        return g.at[k, q, :, point(i), owner(i)]

    def half(q, part, i):
        return g.at[c, q, part, point(i), owner(i)]

    def z_copy(i):
        target = to_energy(offset(i))
        return pltpu.make_async_remote_copy(
            src_ref=own_rows(point(i), target),
            dst_ref=g.at[c, o, :, point(i), e],
            send_sem=zsend.at[i - points],
            recv_sem=zrecv.at[i - points],
            device_id={"energy": target},
            device_id_type=MESH,
        )

    def z_arrival(i):
        tile_ref = block(c, o, i)
        return pltpu.make_async_remote_copy(
            src_ref=tile_ref,
            dst_ref=tile_ref,
            send_sem=zsend.at[i - points],
            recv_sem=zrecv.at[i - points],
            device_id={"energy": owner(i)},
            device_id_type=MESH,
        )

    def local_copy(s):
        return pltpu.make_async_copy(own_rows(s, e), g.at[c, o, :, s, e], local_sem.at[s])

    def own_copy(way, i, src, dst):
        return pltpu.make_async_remote_copy(
            src_ref=src,
            dst_ref=dst,
            send_sem=osend.at[way, i],
            recv_sem=orecv.at[way, i],
            device_id=(to_x, to_y)[way],
            device_id_type=MESH,
        )

    def own_arrival(way, i):
        tile_ref = block(c, (ox, oy)[way], i)
        return own_copy(way, i, tile_ref, tile_ref)

    def move(kind, i, ref):
        return pltpu.make_async_remote_copy(
            src_ref=ref,
            dst_ref=ref,
            send_sem=send.at[kind, i],
            recv_sem=recv.at[kind, i],
            device_id={DA: to_y, DB: to_x}.get(kind, to_peer),
            device_id_type=MESH,
        )

    def outgoing(kind, i):
        refs = {
            P0: lambda: block(c, o, i),
            DA: lambda: half(ox, 0, i),
            PX: lambda: block(c, ox, i),
            DB: lambda: half(oy, 1, i),
            PY: lambda: block(c, oy, i),
            PD: lambda: block(c, od, i),
        }
        return move(kind, i, refs[kind]())

    def incoming(kind, i):
        refs = {
            DA: lambda: half(od, 0, i),
            DB: lambda: half(od, 1, i),
            P0: lambda: block(cp, o, i),
            PX: lambda: block(cp, ox, i),
            PY: lambda: block(cp, oy, i),
            PD: lambda: block(cp, od, i),
        }
        return move(kind, i, refs[kind]())

    def locals_start(s, _):
        local_copy(s).start()
        return 0

    barrier = pltpu.get_barrier_semaphore()
    for d in range(1, nz):
        pl.semaphore_signal(barrier, inc=1, device_id={"energy": to_energy(d)}, device_id_type=MESH)
    for target in (to_x, to_y, to_peer):
        pl.semaphore_signal(barrier, inc=1, device_id=target, device_id_type=MESH)
    lax.fori_loop(0, points, locals_start, 0)
    map_copy = pltpu.make_async_copy(map_hbm, map_ref, map_sem)
    map_copy.start()
    u_copy = pltpu.make_async_copy(coupling, u, u_sem)
    u_copy.start()
    pl.semaphore_wait(barrier, nz - 1 + 3)

    def first_start(s, _):
        dst = g.at[c, o, :, s, e]
        own_copy(0, s, own_rows(s, e), dst).start()
        own_copy(1, s, own_rows(s, e), dst).start()
        z_copy(points + s).start()
        return 0

    def z_start(i, _):
        z_copy(i).start()
        return 0

    lax.fori_loop(0, points, first_start, 0)
    lax.fori_loop(2 * points, ticks, z_start, 0)

    acc[...] = jnp.zeros(acc.shape, acc.dtype)
    map_copy.wait()
    u_copy.wait()

    def multiply(chunks, i, store):
        s = point(i)
        z = owner(i)

        def one(t, _):
            lhs, rhs = [], []
            for k, q in chunks:
                lhs.append(g[k, q, 0, s, z])
                lhs.append(g[k, q, 1, s, z])
                index = map_ref[c * points + t, k * points + s]
                at = pl.ds(pl.multiple_of(q * width, width), width)
                ur = u[0, index, at, :]
                ui = u[1, index, at, :]
                rhs.append(jnp.concatenate([ur, ui], axis=1))
                rhs.append(jnp.concatenate([-ui, ur], axis=1))
            store(
                t,
                acc[t]
                + jnp.dot(
                    jnp.concatenate(lhs, axis=1),
                    jnp.concatenate(rhs, axis=0),
                    preferred_element_type=jnp.float32,
                ),
            )
            return 0

        lax.fori_loop(0, points, one, 0, unroll=True)

    def add(t, values):
        acc[t] = values

    def write(z):
        def store(t, values):
            for part in range(2):
                out[part, z, t, 0] = values[:, part * width : (part + 1) * width].astype(out.dtype)

        return store

    def drain(i):
        @pl.when(i >= points)
        def _():
            z_copy(i).wait_send()

        own_arrival(0, i).wait_send()
        own_arrival(1, i).wait_send()
        for kind in range(6):
            outgoing(kind, i).wait_send()

    def lagged(i, lag):
        return pl.when((i >= lag) & (i < ticks + lag))

    early = ((c, o), (cp, o), (c, ox), (cp, ox), (c, oy), (cp, oy))
    late = ((c, od), (cp, od))

    def arrive(i, kinds):
        for kind in kinds:
            incoming(kind, i).wait_recv()

    def relay(r):
        own_arrival(0, r).wait_recv()
        outgoing(DA, r).start()
        outgoing(PX, r).start()
        own_arrival(1, r).wait_recv()
        outgoing(DB, r).start()
        outgoing(PY, r).start()

    def diagonal(r):
        arrive(r, (DA, DB))
        outgoing(PD, r).start()

    def tick(i, _):
        @pl.when(i < points)
        def _():
            local_copy(point(i)).wait()
            outgoing(P0, i).start()

        @pl.when((i >= points) & (i < ticks))
        def _():
            z_arrival(i).wait_recv()
            for way in range(2):
                own_copy(way, i, block(c, o, i), block(c, o, i)).start()
            outgoing(P0, i).start()

        @lagged(i, RELAY)
        def _():
            relay(i - RELAY)

        @lagged(i, DIAG)
        def _():
            diagonal(i - DIAG)

        @pl.when(i >= MULTIPLY)
        def _():
            r = i - MULTIPLY
            arrive(r, (P0, PX, PY, PD))
            multiply(early + late, r, add)
            drain(r)

            @pl.when(point(r) == points - 1)
            def _():
                z = owner(r)

                def flush(t, _):
                    write(z)(t, acc[t])
                    acc[t] = jnp.zeros(acc.shape[1:], acc.dtype)
                    return 0

                lax.fori_loop(0, points, flush, 0, unroll=True)

        return 0

    lax.fori_loop(0, ticks + MULTIPLY - 1, tick, 0)
    last = ticks - 1
    arrive(last, (P0, PX, PY))
    multiply(early, last, add)
    arrive(last, (PD,))
    multiply(late, last, write(owner(last)))
    drain(last)


def per_device_fused(nz, lesser, coupling, transfer_map):
    points = lesser.shape[2]
    tile = lesser.shape[4] // nz
    width = lesser.shape[5]
    out_cols = coupling.shape[3]
    dma = pltpu.SemaphoreType.DMA
    lesser, coupling, transfer_map = (
        pltpu.with_memory_space_constraint(x, pltpu.HBM) for x in (lesser, coupling, transfer_map)
    )
    return pl.pallas_call(
        functools.partial(kernel, nz),
        out_shape=jax.ShapeDtypeStruct((2, nz, points, 1, tile, out_cols), jnp.bfloat16),
        in_specs=[pl.BlockSpec(memory_space=pltpu.HBM)] * 3,
        out_specs=pl.BlockSpec(memory_space=pltpu.VMEM),
        scratch_shapes=[
            pltpu.VMEM((2, 4, 2, points, nz, tile, width), lesser.dtype),
            pltpu.VMEM(coupling.shape, coupling.dtype),
            pltpu.VMEM((points, tile, 2 * out_cols), jnp.float32),
            pltpu.SMEM(transfer_map.shape, transfer_map.dtype),
            dma(((nz - 1) * points,)),
            dma(((nz - 1) * points,)),
            dma((2, nz * points)),
            dma((2, nz * points)),
            dma((6, nz * points)),
            dma((6, nz * points)),
            dma((points,)),
            dma(()),
            dma(()),
        ],
        compiler_params=pltpu.CompilerParams(
            collective_id=0, has_side_effects=True, vmem_limit_bytes=40 * 1024 * 1024
        ),
    )(transfer_map, lesser, coupling)


def solution(mesh):
    in_specs = (P(None, "energy", "kpt", None, None, "orb"), P(None, None, None, "orb"), P())
    out_specs = P(None, None, "kpt", None, "energy", "orb")
    nz = mesh.shape["energy"]

    def per_device(lesser, coupling, transfer_map):
        shape = lesser.shape
        fused = (
            mesh.shape["orb"] == 4
            and mesh.shape["kpt"] == 2
            and nz > 1
            and shape[1] == 1
            and shape[3] == 1
            and shape[5] == coupling.shape[3] == 128
            and shape[4] == nz * 128
        )
        if fused:
            return per_device_fused(nz, lesser, coupling, transfer_map)
        return per_device_general(lesser, coupling, transfer_map)

    return jax.shard_map(
        per_device, mesh=mesh, in_specs=in_specs, out_specs=out_specs, check_vma=False
    )
```

```python
import functools

import jax
import jax.numpy as jnp
from jax import lax
from jax.experimental import pallas as pl
from jax.experimental.pallas import tpu as pltpu
from jax.sharding import PartitionSpec as P

MESH = pl.DeviceIdType.MESH
LEAD, RELAY, EARLY, DIAG, LATE = 3, 2, 3, 4, 5
SLOTS = 8
GROUPS = 2
PACE = 5


def complex_terms(green, selected):
    real_out = jnp.einsum(
        "prm,tpmj->trj", green[0], selected[0], preferred_element_type=jnp.float32
    ) - jnp.einsum("prm,tpmj->trj", green[1], selected[1], preferred_element_type=jnp.float32)
    imag_out = jnp.einsum(
        "prm,tpmj->trj", green[0], selected[1], preferred_element_type=jnp.float32
    ) + jnp.einsum("prm,tpmj->trj", green[1], selected[0], preferred_element_type=jnp.float32)
    return (real_out, imag_out)


def per_device_general(lesser, coupling, transfer_map):
    regrouped = lax.all_to_all(lesser, "energy", split_axis=4, concat_axis=1, tiled=True)
    gathered = lax.all_gather(regrouped, "orb", axis=5, tiled=True)
    energies = gathered.shape[1]
    local_points = gathered.shape[2]
    layers = gathered.shape[3]
    tile = gathered.shape[4]
    width = gathered.shape[5]
    out_cols = coupling.shape[3]
    row_count = energies * layers * tile
    first_point = lax.axis_index("kpt") * local_points
    reordered = jnp.moveaxis(gathered, 2, 1).reshape(2, local_points, row_count, width)
    my_columns = lax.dynamic_slice_in_dim(transfer_map, first_point, local_points, 1)
    selected = jnp.take(coupling, my_columns, axis=1)
    real_out, imag_out = complex_terms(reordered, selected)
    mine = lax.psum_scatter(
        jnp.stack([real_out, imag_out], axis=1), "kpt", scatter_dimension=0, tiled=True
    )
    summed = jnp.moveaxis(mine, 1, 0)
    result = summed.astype(jnp.bfloat16).reshape(2, local_points, energies, layers, tile, out_cols)
    return jnp.moveaxis(result, 1, 2)


def kernel(nz, map_hbm, lesser, coupling, out, g, u, acc, map_ref, sems, zsend, zrecv, far, local_sem, u_sem, map_sem):
    osend, orecv, fsend, frecv, psend, precv, qrecv = (sems.at[n] for n in range(7))
    points = lesser.shape[2]
    width = lesser.shape[5]
    tile = g.shape[5]
    ticks = nz * points
    bunch = points // GROUPS
    e = lax.axis_index("energy")
    o = lax.axis_index("orb")
    c = lax.axis_index("kpt")
    ox = o + 1 - 2 * lax.rem(o, 2)
    oy = lax.rem(o + 2, 4)
    od = 3 - o
    cp = 1 - c
    to_x, to_y, to_peer = {"orb": ox}, {"orb": oy}, {"kpt": cp}

    def phase(i):
        return lax.div(i, points)

    def point(i):
        return lax.rem(i, points)

    def slot(i):
        return lax.rem(i, SLOTS)

    def offset(p):
        near = lax.div(p + 1, 2)
        return lax.select(lax.rem(p, 2) == 1, near, lax.rem(nz - lax.div(p, 2), nz))

    def owner(i):
        return lax.rem(e + nz - offset(phase(i)), nz)

    def rows(z):
        return pl.ds(pl.multiple_of(z * tile, tile), tile)

    def block(k, q, i):
        return g.at[k, q, :, point(i), owner(i)]

    def remote(src, dst, send_sem, recv_sem, target):
        return pltpu.make_async_remote_copy(
            src_ref=src,
            dst_ref=dst,
            send_sem=send_sem,
            recv_sem=recv_sem,
            device_id=target,
            device_id_type=MESH,
        )

    def z_copy(n):
        p = lax.div(n, GROUPS) + 1
        some = pl.ds(lax.rem(n, GROUPS) * bunch, bunch)
        target = lax.rem(e + offset(p), nz)
        return remote(
            lesser.at[:, 0, some, 0, rows(target), :],
            g.at[c, o, :, some, e],
            zsend.at[n],
            zrecv.at[n],
            {"energy": target},
        )

    def z_arrival(n):
        p = lax.div(n, GROUPS) + 1
        some = pl.ds(lax.rem(n, GROUPS) * bunch, bunch)
        source = lax.rem(e + nz - offset(p), nz)
        ref = g.at[c, o, :, some, source]
        return remote(ref, ref, zsend.at[n], zrecv.at[n], {"energy": source})

    local_copy = pltpu.make_async_copy(
        lesser.at[:, 0, :, 0, rows(e), :], g.at[c, o, :, :, e], local_sem
    )

    def own_start(i, src):
        for target in (to_x, to_y):
            remote(src, block(c, o, i), osend.at[slot(i)], orecv.at[slot(i)], target).start()

    def own_both(i):
        ref = g.at[c, pl.ds(0, 2), :, point(i), owner(i)]
        return remote(ref, ref, osend.at[slot(i)], orecv.at[slot(i)], to_x)

    def relay_start(i):
        for part, q, target in ((0, ox, to_y), (1, oy, to_x)):
            ref = g.at[c, q, part, point(i), owner(i)]
            remote(ref, ref, fsend.at[slot(i)], frecv.at[slot(i)], target).start()

    def relay_both(i):
        ref = block(c, od, i)
        return remote(ref, ref, fsend.at[slot(i)], frecv.at[slot(i)], to_x)

    def peer_start(i, q, recv):
        ref = block(c, q, i)
        remote(ref, ref, psend.at[slot(i)], recv.at[slot(i)], to_peer).start()

    def peer_some(i, count, recv):
        ref = g.at[cp, pl.ds(0, count), :, point(i), owner(i)]
        return remote(ref, ref, psend.at[slot(i)], recv.at[slot(i)], to_peer)

    barrier = pltpu.get_barrier_semaphore()
    has_low, has_high = e > 0, e < nz - 1
    for target in (to_x, to_y, to_peer):
        pl.semaphore_signal(barrier, inc=1, device_id=target, device_id_type=MESH)

    def signal(sem, target, wanted):
        @pl.when(wanted)
        def _():
            pl.semaphore_signal(sem, inc=1, device_id={"energy": target}, device_id_type=MESH)

    signal(barrier, e - 1, has_low)
    signal(barrier, e + 1, has_high)
    local_copy.start()
    map_copy = pltpu.make_async_copy(map_hbm, map_ref, map_sem)
    map_copy.start()
    u_copy = pltpu.make_async_copy(coupling, u, u_sem)
    u_copy.start()
    pl.semaphore_wait(barrier, 3 + has_low.astype(jnp.int32) + has_high.astype(jnp.int32))

    for i in range(LEAD):
        own_start(i, lesser.at[:, 0, i, 0, rows(e), :])

    for h in range(nz - 2):
        signal(far.at[0, h], e - 1, has_low & (e + h + 1 < nz))
        signal(far.at[1, h], e + 1, has_high & (e - h - 1 >= 0))

        @pl.when(e + h + 2 < nz)
        def _(h=h):
            pl.semaphore_wait(far.at[0, h], 1)

        @pl.when(e - h - 2 >= 0)
        def _(h=h):
            pl.semaphore_wait(far.at[1, h], 1)

    def z_start(n, _):
        z_copy(n).start()
        return 0

    z_groups = (nz - 1) * GROUPS
    lax.fori_loop(0, GROUPS, z_start, 0)
    acc[...] = jnp.zeros(acc.shape, acc.dtype)
    local_copy.wait()
    map_copy.wait()
    u_copy.wait()

    def multiply(chunks, i, store):
        s = point(i)
        z = owner(i)
        half = lax.rem(phase(i), 2)

        def one(t, _):
            lhs, rhs = [], []
            for k, q in chunks:
                lhs.append(g[k, q, 0, s, z])
                lhs.append(g[k, q, 1, s, z])
                index = map_ref[c * points + t, k * points + s]
                at = pl.ds(pl.multiple_of(q * width, width), width)
                ur = u[0, index, at, :]
                ui = u[1, index, at, :]
                rhs.append(jnp.concatenate([ur, ui], axis=1))
                rhs.append(jnp.concatenate([-ui, ur], axis=1))
            product = jnp.dot(
                jnp.concatenate(lhs, axis=1),
                jnp.concatenate(rhs, axis=0),
                preferred_element_type=jnp.float32,
            )
            store(half, z, t, acc[half, t] + product)
            return 0

        lax.fori_loop(0, points, one, 0, unroll=True)

    def add(half, z, t, values):
        acc[half, t] = values

    def write(half, z, t, values):
        for part in range(2):
            out[part, z, t, 0] = values[:, part * width : (part + 1) * width].astype(out.dtype)

    early = ((c, o), (cp, o), (c, ox), (cp, ox), (c, oy), (cp, oy))
    late = ((c, od), (cp, od))

    def lagged(i, lag):
        return pl.when((i >= lag) & (i < ticks + lag))

    def drain(r):
        own_both(r).wait_send()
        relay_both(r).wait_send()
        peer_some(r, 4, precv).wait_send()

    def tick(i, _):
        @pl.when((i > 0) & (i <= (nz - 2) * PACE) & (lax.rem(i, PACE) == 0))
        def _():
            n = lax.div(i, PACE) * GROUPS
            lax.fori_loop(n, n + GROUPS, z_start, 0)

        @pl.when((i >= points) & (i < ticks) & (lax.rem(i, bunch) == 0))
        def _():
            z_arrival(lax.div(i - points, bunch)).wait_recv()

        @pl.when((i >= LEAD) & (i < ticks))
        def _():
            own_start(i, block(c, o, i))

        @lagged(i, 0)
        def _():
            peer_start(i, o, precv)

        @lagged(i, RELAY)
        def _():
            r = i - RELAY
            own_both(r).wait_recv()
            relay_start(r)
            peer_start(r, ox, precv)
            peer_start(r, oy, precv)

        @lagged(i, DIAG)
        def _():
            r = i - DIAG
            relay_both(r).wait_recv()
            peer_start(r, od, qrecv)

        @lagged(i, EARLY)
        def _():
            r = i - EARLY
            peer_some(r, 3, precv).wait_recv()
            multiply(early, r, add)

        @pl.when(i >= LATE)
        def _():
            r = i - LATE
            peer_some(r, 1, qrecv).wait_recv()
            multiply(late, r, add)
            drain(r)

            @pl.when(point(r) == points - 1)
            def _():
                half = lax.rem(phase(r), 2)

                def flush(t, _):
                    write(half, owner(r), t, acc[half, t])
                    acc[half, t] = jnp.zeros(acc.shape[2:], acc.dtype)
                    return 0

                lax.fori_loop(0, points, flush, 0, unroll=True)

        return 0

    lax.fori_loop(0, ticks + LATE - 1, tick, 0)
    last = ticks - 1
    peer_some(last, 1, qrecv).wait_recv()
    multiply(late, last, write)
    drain(last)

    def z_drain(n, _):
        z_copy(n).wait_send()
        return 0

    lax.fori_loop(0, z_groups, z_drain, 0)


def per_device_fused(nz, lesser, coupling, transfer_map):
    points = lesser.shape[2]
    tile = lesser.shape[4] // nz
    width = lesser.shape[5]
    out_cols = coupling.shape[3]
    dma = pltpu.SemaphoreType.DMA
    lesser, coupling, transfer_map = (
        pltpu.with_memory_space_constraint(x, pltpu.HBM) for x in (lesser, coupling, transfer_map)
    )
    return pl.pallas_call(
        functools.partial(kernel, nz),
        out_shape=jax.ShapeDtypeStruct((2, nz, points, 1, tile, out_cols), jnp.bfloat16),
        in_specs=[pl.BlockSpec(memory_space=pltpu.HBM)] * 3,
        out_specs=pl.BlockSpec(memory_space=pltpu.VMEM),
        scratch_shapes=[
            pltpu.VMEM((2, 4, 2, points, nz, tile, width), lesser.dtype),
            pltpu.VMEM(coupling.shape, coupling.dtype),
            pltpu.VMEM((2, points, tile, 2 * out_cols), jnp.float32),
            pltpu.SMEM(transfer_map.shape, transfer_map.dtype),
            dma((7, SLOTS)),
            dma(((nz - 1) * GROUPS,)),
            dma(((nz - 1) * GROUPS,)),
            pltpu.SemaphoreType.REGULAR((2, max(nz - 2, 1))),
            dma(()),
            dma(()),
            dma(()),
        ],
        compiler_params=pltpu.CompilerParams(
            collective_id=0, has_side_effects=True, vmem_limit_bytes=40 * 1024 * 1024
        ),
    )(transfer_map, lesser, coupling)


def solution(mesh):
    in_specs = (P(None, "energy", "kpt", None, None, "orb"), P(None, None, None, "orb"), P())
    out_specs = P(None, None, "kpt", None, "energy", "orb")
    nz = mesh.shape["energy"]

    def per_device(lesser, coupling, transfer_map):
        shape = lesser.shape
        fused = (
            mesh.shape["orb"] == 4
            and mesh.shape["kpt"] == 2
            and nz > 1
            and shape[1] == 1
            and shape[3] == 1
            and shape[5] == coupling.shape[3] == 128
            and shape[4] == nz * 128
            and shape[2] % GROUPS == 0
            and nz * shape[2] > LEAD
            and PACE <= shape[2]
        )
        if fused:
            return per_device_fused(nz, lesser, coupling, transfer_map)
        return per_device_general(lesser, coupling, transfer_map)

    return jax.shard_map(
        per_device, mesh=mesh, in_specs=in_specs, out_specs=out_specs, check_vma=False
    )
```

```python
import functools

import jax
import jax.numpy as jnp
from jax import lax
from jax.experimental import pallas as pl
from jax.experimental.pallas import tpu as pltpu
from jax.sharding import PartitionSpec as P

MESH = pl.DeviceIdType.MESH
LEAD, RELAY, EARLY, DIAG, LATE = 4, 2, 3, 5, 6
ADVANCE = 26
CATCH_UP = 12
SLOTS = 8
GROUPS = 2
PACE = 5


def complex_terms(green, selected):
    real_out = jnp.einsum(
        "prm,tpmj->trj", green[0], selected[0], preferred_element_type=jnp.float32
    ) - jnp.einsum("prm,tpmj->trj", green[1], selected[1], preferred_element_type=jnp.float32)
    imag_out = jnp.einsum(
        "prm,tpmj->trj", green[0], selected[1], preferred_element_type=jnp.float32
    ) + jnp.einsum("prm,tpmj->trj", green[1], selected[0], preferred_element_type=jnp.float32)
    return (real_out, imag_out)


def per_device_general(lesser, coupling, transfer_map):
    regrouped = lax.all_to_all(lesser, "energy", split_axis=4, concat_axis=1, tiled=True)
    gathered = lax.all_gather(regrouped, "orb", axis=5, tiled=True)
    energies = gathered.shape[1]
    local_points = gathered.shape[2]
    layers = gathered.shape[3]
    tile = gathered.shape[4]
    width = gathered.shape[5]
    out_cols = coupling.shape[3]
    row_count = energies * layers * tile
    first_point = lax.axis_index("kpt") * local_points
    reordered = jnp.moveaxis(gathered, 2, 1).reshape(2, local_points, row_count, width)
    my_columns = lax.dynamic_slice_in_dim(transfer_map, first_point, local_points, 1)
    selected = jnp.take(coupling, my_columns, axis=1)
    real_out, imag_out = complex_terms(reordered, selected)
    mine = lax.psum_scatter(
        jnp.stack([real_out, imag_out], axis=1), "kpt", scatter_dimension=0, tiled=True
    )
    summed = jnp.moveaxis(mine, 1, 0)
    result = summed.astype(jnp.bfloat16).reshape(2, local_points, energies, layers, tile, out_cols)
    return jnp.moveaxis(result, 1, 2)


def kernel(nz, map_hbm, lesser, coupling, out, g, u, acc, map_ref, sems, zsend, zrecv, far, local_sem, u_sem, map_sem):
    sent, orecv, frecv, precv, qrecv = (sems.at[n] for n in range(5))
    points = lesser.shape[2]
    width = lesser.shape[5]
    tile = g.shape[5]
    copies = 7
    ticks = nz * points
    bunch = points // GROUPS
    e = lax.axis_index("energy")
    o = lax.axis_index("orb")
    c = lax.axis_index("kpt")
    ox = o + 1 - 2 * lax.rem(o, 2)
    oy = lax.rem(o + 2, 4)
    od = 3 - o
    cp = 1 - c
    to_x, to_y, to_peer = {"orb": ox}, {"orb": oy}, {"kpt": cp}

    def phase(i):
        return lax.div(i, points)

    def point(i):
        return lax.rem(i, points)

    def slot(i):
        return lax.rem(i, SLOTS)

    def offset(p):
        near = lax.div(p + 1, 2)
        return lax.select(lax.rem(p, 2) == 1, near, lax.rem(nz - lax.div(p, 2), nz))

    def owner(i):
        return lax.rem(e + nz - offset(phase(i)), nz)

    def rows(z):
        return pl.ds(pl.multiple_of(z * tile, tile), tile)

    def block(k, q, i):
        return g.at[k, q, point(i), owner(i)]

    def remote(src, dst, send_sem, recv_sem, target):
        return pltpu.make_async_remote_copy(
            src_ref=src,
            dst_ref=dst,
            send_sem=send_sem,
            recv_sem=recv_sem,
            device_id=target,
            device_id_type=MESH,
        )

    def z_start(n, _):
        p = lax.div(n, GROUPS) + 1
        some = pl.ds(lax.rem(n, GROUPS) * bunch, bunch)
        target = lax.rem(e + offset(p), nz)
        for part in range(2):
            remote(
                lesser.at[part, 0, some, 0, rows(target), :],
                g.at[c, o, some, e, part],
                zsend,
                zrecv.at[n],
                {"energy": target},
            ).start()
        return 0

    def z_arrival(n):
        ref = g.at[c, o, pl.ds(0, bunch), 0]
        return remote(ref, ref, zsend, zrecv.at[n], to_x)

    def z_sent():
        ref = g.at[c, pl.ds(0, nz - 1), :, 0]
        return remote(ref, ref, zsend, zrecv.at[0], to_x)

    def local_copy(part):
        return pltpu.make_async_copy(
            lesser.at[part, 0, :, 0, rows(e), :], g.at[c, o, :, e, part], local_sem.at[part]
        )

    def own_start(i):
        ref = block(c, o, i)
        for target in (to_x, to_y):
            remote(ref, ref, sent.at[slot(i)], orecv.at[slot(i)], target).start()

    def own_both(i):
        ref = g.at[c, pl.ds(0, 2), point(i), owner(i)]
        return remote(ref, ref, sent.at[slot(i)], orecv.at[slot(i)], to_x)

    def relay_start(i):
        for part, q, target in ((0, ox, to_y), (1, oy, to_x)):
            ref = g.at[c, q, point(i), owner(i), part]
            remote(ref, ref, sent.at[slot(i)], frecv.at[slot(i)], target).start()

    def relay_both(i):
        ref = block(c, od, i)
        return remote(ref, ref, sent.at[slot(i)], frecv.at[slot(i)], to_x)

    def all_sent(i):
        ref = g.at[c, o, pl.ds(0, copies), 0]
        return remote(ref, ref, sent.at[slot(i)], orecv.at[slot(i)], to_x)

    def peer_start(i, q, recv):
        ref = block(c, q, i)
        remote(ref, ref, sent.at[slot(i)], recv.at[slot(i)], to_peer).start()

    def peer_some(i, count, recv):
        ref = g.at[cp, pl.ds(0, count), point(i), owner(i)]
        return remote(ref, ref, sent.at[slot(i)], recv.at[slot(i)], to_peer)

    barrier = pltpu.get_barrier_semaphore()
    has_low, has_high = e > 0, e < nz - 1
    for target in (to_x, to_y, to_peer):
        pl.semaphore_signal(barrier, inc=1, device_id=target, device_id_type=MESH)

    def signal(sem, target, wanted):
        @pl.when(wanted)
        def _():
            pl.semaphore_signal(sem, inc=1, device_id={"energy": target}, device_id_type=MESH)

    signal(barrier, e - 1, has_low)
    signal(barrier, e + 1, has_high)
    for part in range(2):
        local_copy(part).start()
    map_copy = pltpu.make_async_copy(map_hbm, map_ref, map_sem)
    map_copy.start()
    u_copy = pltpu.make_async_copy(coupling, u, u_sem)
    u_copy.start()
    pl.semaphore_wait(barrier, 3 + has_low.astype(jnp.int32) + has_high.astype(jnp.int32))

    for part in range(2):
        local_copy(part).wait()
    for i in range(LEAD):
        own_start(i)
        peer_start(i, o, precv)

    for h in range(nz - 2):
        signal(far.at[0, h], e - 1, has_low & (e + h + 1 < nz))
        signal(far.at[1, h], e + 1, has_high & (e - h - 1 >= 0))

        @pl.when(e + h + 2 < nz)
        def _(h=h):
            pl.semaphore_wait(far.at[0, h], 1)

        @pl.when(e - h - 2 >= 0)
        def _(h=h):
            pl.semaphore_wait(far.at[1, h], 1)

    lax.fori_loop(0, GROUPS, z_start, 0)
    acc[...] = jnp.zeros(acc.shape, acc.dtype)
    map_copy.wait()
    u_copy.wait()

    def multiply(chunks, i, store):
        s = point(i)
        z = owner(i)
        half = lax.rem(phase(i), 2)

        def one(t, _):
            lhs, rhs = [], []
            for k, q in chunks:
                lhs.append(g[k, q, s, z, 0])
                lhs.append(g[k, q, s, z, 1])
                index = map_ref[c * points + t, k * points + s]
                at = pl.ds(pl.multiple_of(q * width, width), width)
                ur = u[0, index, at, :]
                ui = u[1, index, at, :]
                rhs.append(jnp.concatenate([ur, ui], axis=1))
                rhs.append(jnp.concatenate([-ui, ur], axis=1))
            product = jnp.dot(
                jnp.concatenate(lhs, axis=1),
                jnp.concatenate(rhs, axis=0),
                preferred_element_type=jnp.float32,
            )
            store(half, z, t, acc[half, t] + product)
            return 0

        lax.fori_loop(0, points, one, 0, unroll=True)

    def add(half, z, t, values):
        acc[half, t] = values

    def write(half, z, t, values):
        for part in range(2):
            out[part, z, t, 0] = values[:, part * width : (part + 1) * width].astype(out.dtype)

    near_chunks = ((c, o), (cp, o), (c, ox), (cp, ox), (c, oy), (cp, oy))
    far_chunks = ((c, od), (cp, od))

    def relay(r):
        own_both(r).wait_recv()
        relay_start(r)
        peer_start(r, ox, precv)
        peer_start(r, oy, precv)

    def diagonal(r):
        relay_both(r).wait_recv()
        peer_start(r, od, qrecv)

    def early(r):
        peer_some(r, 3, precv).wait_recv()
        multiply(near_chunks, r, add)

    def late(r):
        peer_some(r, 1, qrecv).wait_recv()
        multiply(far_chunks, r, add)
        all_sent(r).wait_send()

        @pl.when(point(r) == points - 1)
        def _():
            half = lax.rem(phase(r), 2)

            def flush(t, _):
                write(half, owner(r), t, acc[half, t])
                acc[half, t] = jnp.zeros(acc.shape[2:], acc.dtype)
                return 0

            lax.fori_loop(0, points, flush, 0, unroll=True)

    def tick(i, _):
        @pl.when((i > 0) & (i <= (nz - 2) * PACE) & (lax.rem(i, PACE) == 0))
        def _():
            n = lax.div(i, PACE) * GROUPS
            lax.fori_loop(n, n + GROUPS, z_start, 0)

        def own(j, _):
            @pl.when((j >= points) & (lax.rem(j, bunch) == 0))
            def _():
                z_arrival(lax.div(j - points, bunch)).wait_recv()

            own_start(j)
            peer_start(j, o, precv)
            return 0

        def lead(j):
            return lax.max(lax.min(j + (j >= ADVANCE).astype(jnp.int32), ticks), LEAD)

        lax.fori_loop(lead(i), lead(i + 1), own, 0)

        @pl.when(i >= RELAY)
        def _():
            relay(i - RELAY)

        @pl.when(i >= DIAG)
        def _():
            diagonal(i - DIAG)

        def one(r, _):
            early(r)
            return 0

        slow, slow_next = ((j < CATCH_UP).astype(jnp.int32) for j in (i, i + 1))
        lax.fori_loop(lax.max(i - EARLY - slow, 0), lax.max(i + 1 - EARLY - slow_next, 0), one, 0)

        @pl.when(i >= LATE)
        def _():
            late(i - LATE)

        return 0

    lax.fori_loop(0, ticks + 1, tick, 0)
    last = ticks - 1
    relay(last)
    early(last - 1)
    diagonal(last - 3)
    late(last - 4)
    diagonal(last - 2)
    late(last - 3)
    diagonal(last - 1)
    early(last)
    diagonal(last)
    late(last - 2)
    late(last - 1)
    peer_some(last, 1, qrecv).wait_recv()
    multiply(far_chunks, last, write)
    all_sent(last).wait_send()
    z_sent().wait_send()


def per_device_fused(nz, lesser, coupling, transfer_map):
    points = lesser.shape[2]
    tile = lesser.shape[4] // nz
    width = lesser.shape[5]
    out_cols = coupling.shape[3]
    dma = pltpu.SemaphoreType.DMA
    lesser, coupling, transfer_map = (
        pltpu.with_memory_space_constraint(x, pltpu.HBM) for x in (lesser, coupling, transfer_map)
    )
    return pl.pallas_call(
        functools.partial(kernel, nz),
        out_shape=jax.ShapeDtypeStruct((2, nz, points, 1, tile, out_cols), jnp.bfloat16),
        in_specs=[pl.BlockSpec(memory_space=pltpu.HBM)] * 3,
        out_specs=pl.BlockSpec(memory_space=pltpu.VMEM),
        scratch_shapes=[
            pltpu.VMEM((2, 4, points, nz, 2, tile, width), lesser.dtype),
            pltpu.VMEM(coupling.shape, coupling.dtype),
            pltpu.VMEM((2, points, tile, 2 * out_cols), jnp.float32),
            pltpu.SMEM(transfer_map.shape, transfer_map.dtype),
            dma((5, SLOTS)),
            dma(()),
            dma(((nz - 1) * GROUPS,)),
            pltpu.SemaphoreType.REGULAR((2, max(nz - 2, 1))),
            dma((2,)),
            dma(()),
            dma(()),
        ],
        compiler_params=pltpu.CompilerParams(
            collective_id=0, has_side_effects=True, vmem_limit_bytes=40 * 1024 * 1024
        ),
    )(transfer_map, lesser, coupling)


def solution(mesh):
    in_specs = (P(None, "energy", "kpt", None, None, "orb"), P(None, None, None, "orb"), P())
    out_specs = P(None, None, "kpt", None, "energy", "orb")
    nz = mesh.shape["energy"]

    def per_device(lesser, coupling, transfer_map):
        shape = lesser.shape
        fused = (
            mesh.shape["orb"] == 4
            and mesh.shape["kpt"] == 2
            and nz > 1
            and shape[1] == 1
            and shape[3] == 1
            and shape[5] == coupling.shape[3] == 128
            and shape[4] == nz * 128
            and shape[2] % GROUPS == 0
            and shape[2] % 2 == 0
            and shape[2] >= 8
            and nz <= 5
            and nz * shape[2] > max(CATCH_UP, ADVANCE)
        )
        if fused:
            return per_device_fused(nz, lesser, coupling, transfer_map)
        return per_device_general(lesser, coupling, transfer_map)

    return jax.shard_map(
        per_device, mesh=mesh, in_specs=in_specs, out_specs=out_specs, check_vma=False
    )
```

```python
import functools

import jax
import jax.numpy as jnp
from jax import lax
from jax.experimental import pallas as pl
from jax.experimental.pallas import tpu as pltpu
from jax.sharding import PartitionSpec as P

MESH = pl.DeviceIdType.MESH
LEAD, RELAY, EARLY, DIAG, LATE = 4, 2, 3, 5, 6
ADVANCE = (24,27)
DEEPER = 25
CATCH_UP = 12
SLOTS = 10
FIRST = 2
GROUPS = 2
PACE = 5


def complex_terms(green, selected):
    real_out = jnp.einsum(
        "prm,tpmj->trj", green[0], selected[0], preferred_element_type=jnp.float32
    ) - jnp.einsum("prm,tpmj->trj", green[1], selected[1], preferred_element_type=jnp.float32)
    imag_out = jnp.einsum(
        "prm,tpmj->trj", green[0], selected[1], preferred_element_type=jnp.float32
    ) + jnp.einsum("prm,tpmj->trj", green[1], selected[0], preferred_element_type=jnp.float32)
    return (real_out, imag_out)


def per_device_general(lesser, coupling, transfer_map):
    regrouped = lax.all_to_all(lesser, "energy", split_axis=4, concat_axis=1, tiled=True)
    gathered = lax.all_gather(regrouped, "orb", axis=5, tiled=True)
    energies = gathered.shape[1]
    local_points = gathered.shape[2]
    layers = gathered.shape[3]
    tile = gathered.shape[4]
    width = gathered.shape[5]
    out_cols = coupling.shape[3]
    row_count = energies * layers * tile
    first_point = lax.axis_index("kpt") * local_points
    reordered = jnp.moveaxis(gathered, 2, 1).reshape(2, local_points, row_count, width)
    my_columns = lax.dynamic_slice_in_dim(transfer_map, first_point, local_points, 1)
    selected = jnp.take(coupling, my_columns, axis=1)
    real_out, imag_out = complex_terms(reordered, selected)
    mine = lax.psum_scatter(
        jnp.stack([real_out, imag_out], axis=1), "kpt", scatter_dimension=0, tiled=True
    )
    summed = jnp.moveaxis(mine, 1, 0)
    result = summed.astype(jnp.bfloat16).reshape(2, local_points, energies, layers, tile, out_cols)
    return jnp.moveaxis(result, 1, 2)


def kernel(nz, map_hbm, lesser, coupling, out, g, u, acc, map_ref, sems, sent, zsend, zrecv, far, local_sem, u_sem, map_sem):
    orecv, frecv, precv, qrecv = (sems.at[n] for n in range(4))
    points = lesser.shape[2]
    width = lesser.shape[5]
    tile = g.shape[5]
    copies = 7
    ticks = nz * points
    bunch = points // GROUPS
    e = lax.axis_index("energy")
    o = lax.axis_index("orb")
    c = lax.axis_index("kpt")
    ox = o + 1 - 2 * lax.rem(o, 2)
    oy = lax.rem(o + 2, 4)
    od = 3 - o
    cp = 1 - c
    to_x, to_y, to_peer = {"orb": ox}, {"orb": oy}, {"kpt": cp}

    def phase(i):
        return lax.div(i, points)

    def point(i):
        return lax.rem(i, points)

    def slot(i):
        return lax.rem(i, SLOTS)

    def offset(p):
        near = lax.div(p + 1, 2)
        return lax.select(lax.rem(p, 2) == 1, near, lax.rem(nz - lax.div(p, 2), nz))

    def owner(i):
        return lax.rem(e + nz - offset(phase(i)), nz)

    def rows(z):
        return pl.ds(pl.multiple_of(z * tile, tile), tile)

    def block(k, q, i):
        return g.at[k, q, point(i), owner(i)]

    def remote(src, dst, send_sem, recv_sem, target):
        return pltpu.make_async_remote_copy(
            src_ref=src,
            dst_ref=dst,
            send_sem=send_sem,
            recv_sem=recv_sem,
            device_id=target,
            device_id_type=MESH,
        )

    def z_start(n, _):
        p = lax.div(n, GROUPS) + 1
        some = pl.ds(lax.rem(n, GROUPS) * bunch, bunch)
        target = lax.rem(e + offset(p), nz)
        for part in range(2):
            remote(
                lesser.at[part, 0, some, 0, rows(target), :],
                g.at[c, o, some, e, part],
                zsend,
                zrecv.at[n],
                {"energy": target},
            ).start()
        return 0

    def z_arrival(n):
        ref = g.at[c, o, pl.ds(0, bunch), 0]
        return remote(ref, ref, zsend, zrecv.at[n], to_x)

    def z_sent():
        ref = g.at[c, pl.ds(0, nz - 1), :, 0]
        return remote(ref, ref, zsend, zrecv.at[0], to_x)

    pieces = (pl.ds(0, FIRST), pl.ds(FIRST, points - FIRST))

    def local_start(n):
        for part in range(2):
            pltpu.make_async_copy(
                lesser.at[part, 0, pieces[n], 0, rows(e), :],
                g.at[c, o, pieces[n], e, part],
                local_sem.at[n],
            ).start()

    def local_wait(n):
        ref = g.at[c, o, pieces[n], e]
        pltpu.make_async_copy(ref, ref, local_sem.at[n]).wait()

    def own_start(i):
        ref = block(c, o, i)
        for target in (to_x, to_y):
            remote(ref, ref, sent, orecv.at[slot(i)], target).start()

    def own_both(i):
        ref = g.at[c, pl.ds(0, 2), point(i), owner(i)]
        return remote(ref, ref, sent, orecv.at[slot(i)], to_x)

    def relay_start(i):
        for part, q, target in ((0, ox, to_y), (1, oy, to_x)):
            ref = g.at[c, q, point(i), owner(i), part]
            remote(ref, ref, sent, frecv.at[slot(i)], target).start()

    def relay_both(i):
        ref = block(c, od, i)
        return remote(ref, ref, sent, frecv.at[slot(i)], to_x)

    def all_sent():
        ref = g.at[:, :, :, :, :, pl.ds(0, tile * copies // 8), :]
        return remote(ref, ref, sent, orecv.at[0], to_x)

    def peer_start(i, q, recv):
        ref = block(c, q, i)
        remote(ref, ref, sent, recv.at[slot(i)], to_peer).start()

    def peer_some(i, count, recv):
        ref = g.at[cp, pl.ds(0, count), point(i), owner(i)]
        return remote(ref, ref, sent, recv.at[slot(i)], to_peer)

    barrier = pltpu.get_barrier_semaphore()
    has_low, has_high = e > 0, e < nz - 1
    for target in (to_x, to_y, to_peer):
        pl.semaphore_signal(barrier, inc=1, device_id=target, device_id_type=MESH)

    def signal(sem, target, wanted):
        @pl.when(wanted)
        def _():
            pl.semaphore_signal(sem, inc=1, device_id={"energy": target}, device_id_type=MESH)

    signal(barrier, e - 1, has_low)
    signal(barrier, e + 1, has_high)
    for n in range(2):
        local_start(n)
    map_copy = pltpu.make_async_copy(map_hbm, map_ref, map_sem)
    map_copy.start()
    u_copy = pltpu.make_async_copy(coupling, u, u_sem)
    u_copy.start()
    pl.semaphore_wait(barrier, 3 + has_low.astype(jnp.int32) + has_high.astype(jnp.int32))

    local_wait(0)
    for i in range(LEAD):
        if i == FIRST:
            local_wait(1)
        own_start(i)
        peer_start(i, o, precv)

    for h in range(nz - 2):
        signal(far.at[0, h], e - 1, has_low & (e + h + 1 < nz))
        signal(far.at[1, h], e + 1, has_high & (e - h - 1 >= 0))

        @pl.when(e + h + 2 < nz)
        def _(h=h):
            pl.semaphore_wait(far.at[0, h], 1)

        @pl.when(e - h - 2 >= 0)
        def _(h=h):
            pl.semaphore_wait(far.at[1, h], 1)

    lax.fori_loop(0, GROUPS, z_start, 0)
    acc[...] = jnp.zeros(acc.shape, acc.dtype)
    map_copy.wait()
    u_copy.wait()

    def multiply(chunks, i, store):
        s = point(i)
        z = owner(i)
        half = lax.rem(phase(i), 2)

        def one(t, _):
            lhs, rhs = [], []
            for k, q in chunks:
                lhs.append(g[k, q, s, z, 0])
                lhs.append(g[k, q, s, z, 1])
                index = map_ref[c * points + t, k * points + s]
                at = pl.ds(pl.multiple_of(q * width, width), width)
                ur = u[0, index, at, :]
                ui = u[1, index, at, :]
                rhs.append(jnp.concatenate([ur, ui], axis=1))
                rhs.append(jnp.concatenate([-ui, ur], axis=1))
            product = jnp.dot(
                jnp.concatenate(lhs, axis=1),
                jnp.concatenate(rhs, axis=0),
                preferred_element_type=jnp.float32,
            )
            store(half, z, t, acc[half, t] + product)
            return 0

        lax.fori_loop(0, points, one, 0, unroll=True)

    def add(half, z, t, values):
        acc[half, t] = values

    def write(half, z, t, values):
        for part in range(2):
            out[part, z, t, 0] = values[:, part * width : (part + 1) * width].astype(out.dtype)

    near_chunks = ((c, o), (cp, o), (c, ox), (cp, ox), (c, oy), (cp, oy))
    far_chunks = ((c, od), (cp, od))

    def relay(r):
        own_both(r).wait_recv()
        relay_start(r)
        peer_start(r, ox, precv)
        peer_start(r, oy, precv)

    def diagonal(r):
        relay_both(r).wait_recv()
        peer_start(r, od, qrecv)

    def early(r):
        peer_some(r, 3, precv).wait_recv()
        multiply(near_chunks, r, add)

    def late(r):
        peer_some(r, 1, qrecv).wait_recv()
        multiply(far_chunks, r, add)

        @pl.when(point(r) == points - 1)
        def _():
            half = lax.rem(phase(r), 2)

            def flush(t, _):
                write(half, owner(r), t, acc[half, t])
                acc[half, t] = jnp.zeros(acc.shape[2:], acc.dtype)
                return 0

            lax.fori_loop(0, points, flush, 0, unroll=True)

    def after(i, bound):
        return (i >= bound).astype(jnp.int32)

    def tick(i, _):
        def stage(done, work):
            def one(r, _):
                work(r)
                return 0

            lax.fori_loop(done(i), done(i + 1), one, 0)

        @pl.when((i > 0) & (i <= (nz - 2) * PACE) & (lax.rem(i, PACE) == 0))
        def _():
            n = lax.div(i, PACE) * GROUPS
            lax.fori_loop(n, n + GROUPS, z_start, 0)

        def own(j):
            @pl.when((j >= points) & (lax.rem(j, bunch) == 0))
            def _():
                z_arrival(lax.div(j - points, bunch)).wait_recv()

            own_start(j)
            peer_start(j, o, precv)

        def own_done(j):
            return lax.max(lax.min(j + sum(after(j, a) for a in ADVANCE), ticks), LEAD)

        stage(own_done, own)

        def lagged(lag):
            return lambda j: lax.max(j - lag(j), 0)

        stage(lagged(lambda j: RELAY), relay)
        stage(lagged(lambda j: DIAG + after(j, DEEPER)), diagonal)
        stage(lagged(lambda j: EARLY + 1 - after(j, CATCH_UP)), early)
        stage(lagged(lambda j: LATE + after(j, DEEPER)), late)
        return 0

    lax.fori_loop(0, ticks - 1, tick, 0)
    last = ticks - 1
    relay(last - 2)
    early(last - 3)
    late(last - 7)
    diagonal(last - 6)
    relay(last - 1)
    early(last - 2)
    late(last - 6)
    diagonal(last - 5)
    relay(last)
    early(last - 1)
    diagonal(last - 4)
    late(last - 5)
    diagonal(last - 3)
    early(last)
    diagonal(last - 2)
    late(last - 4)
    diagonal(last - 1)
    late(last - 3)
    diagonal(last)
    late(last - 2)
    late(last - 1)
    peer_some(last, 1, qrecv).wait_recv()
    multiply(far_chunks, last, write)
    all_sent().wait_send()
    z_sent().wait_send()


def per_device_fused(nz, lesser, coupling, transfer_map):
    points = lesser.shape[2]
    tile = lesser.shape[4] // nz
    width = lesser.shape[5]
    out_cols = coupling.shape[3]
    dma = pltpu.SemaphoreType.DMA
    lesser, coupling, transfer_map = (
        pltpu.with_memory_space_constraint(x, pltpu.HBM) for x in (lesser, coupling, transfer_map)
    )
    return pl.pallas_call(
        functools.partial(kernel, nz),
        out_shape=jax.ShapeDtypeStruct((2, nz, points, 1, tile, out_cols), jnp.bfloat16),
        in_specs=[pl.BlockSpec(memory_space=pltpu.HBM)] * 3,
        out_specs=pl.BlockSpec(memory_space=pltpu.VMEM),
        scratch_shapes=[
            pltpu.VMEM((2, 4, points, nz, 2, tile, width), lesser.dtype),
            pltpu.VMEM(coupling.shape, coupling.dtype),
            pltpu.VMEM((2, points, tile, 2 * out_cols), jnp.float32),
            pltpu.SMEM(transfer_map.shape, transfer_map.dtype),
            dma((4, SLOTS)),
            dma(()),
            dma(()),
            dma(((nz - 1) * GROUPS,)),
            pltpu.SemaphoreType.REGULAR((2, max(nz - 2, 1))),
            dma((2,)),
            dma(()),
            dma(()),
        ],
        compiler_params=pltpu.CompilerParams(
            collective_id=0, has_side_effects=True, vmem_limit_bytes=40 * 1024 * 1024
        ),
    )(transfer_map, lesser, coupling)


def solution(mesh):
    in_specs = (P(None, "energy", "kpt", None, None, "orb"), P(None, None, None, "orb"), P())
    out_specs = P(None, None, "kpt", None, "energy", "orb")
    nz = mesh.shape["energy"]

    def per_device(lesser, coupling, transfer_map):
        shape = lesser.shape
        fused = (
            mesh.shape["orb"] == 4
            and mesh.shape["kpt"] == 2
            and nz > 1
            and shape[1] == 1
            and shape[3] == 1
            and shape[5] == coupling.shape[3] == 128
            and shape[4] == nz * 128
            and shape[2] % GROUPS == 0
            and shape[2] % 2 == 0
            and shape[2] >= max(LEAD, PACE)
            and nz * shape[2] > max(CATCH_UP, DEEPER, LATE, *ADVANCE)
        )
        if fused:
            return per_device_fused(nz, lesser, coupling, transfer_map)
        return per_device_general(lesser, coupling, transfer_map)

    return jax.shard_map(
        per_device, mesh=mesh, in_specs=in_specs, out_specs=out_specs, check_vma=False
    )
```

```python
import functools

import jax
import jax.numpy as jnp
from jax import lax
from jax.experimental import pallas as pl
from jax.experimental.pallas import tpu as pltpu
from jax.sharding import PartitionSpec as P

MESH = pl.DeviceIdType.MESH
LEAD, RELAY, EARLY, DIAG, LATE = 5, 2, 3, 5, 6
ADVANCE = (24,27)
DEEPER = 25
CATCH_UP = 12
SLOTS = 10
DIAG_SLOTS = 6
FIRST = 2
GROUPS = 2
PACE = 5


def complex_terms(green, selected):
    real_out = jnp.einsum(
        "prm,tpmj->trj", green[0], selected[0], preferred_element_type=jnp.float32
    ) - jnp.einsum("prm,tpmj->trj", green[1], selected[1], preferred_element_type=jnp.float32)
    imag_out = jnp.einsum(
        "prm,tpmj->trj", green[0], selected[1], preferred_element_type=jnp.float32
    ) + jnp.einsum("prm,tpmj->trj", green[1], selected[0], preferred_element_type=jnp.float32)
    return (real_out, imag_out)


def per_device_general(lesser, coupling, transfer_map):
    regrouped = lax.all_to_all(lesser, "energy", split_axis=4, concat_axis=1, tiled=True)
    gathered = lax.all_gather(regrouped, "orb", axis=5, tiled=True)
    energies = gathered.shape[1]
    local_points = gathered.shape[2]
    layers = gathered.shape[3]
    tile = gathered.shape[4]
    width = gathered.shape[5]
    out_cols = coupling.shape[3]
    row_count = energies * layers * tile
    first_point = lax.axis_index("kpt") * local_points
    reordered = jnp.moveaxis(gathered, 2, 1).reshape(2, local_points, row_count, width)
    my_columns = lax.dynamic_slice_in_dim(transfer_map, first_point, local_points, 1)
    selected = jnp.take(coupling, my_columns, axis=1)
    real_out, imag_out = complex_terms(reordered, selected)
    mine = lax.psum_scatter(
        jnp.stack([real_out, imag_out], axis=1), "kpt", scatter_dimension=0, tiled=True
    )
    summed = jnp.moveaxis(mine, 1, 0)
    result = summed.astype(jnp.bfloat16).reshape(2, local_points, energies, layers, tile, out_cols)
    return jnp.moveaxis(result, 1, 2)


def kernel(nz, map_hbm, lesser, coupling, out, g, u, acc, map_ref, sems, qrecv, sent, zsend, zrecv, far, local_sem, u_sem, map_sem):
    orecv, frecv, precv = (sems.at[n] for n in range(3))
    points = lesser.shape[2]
    width = lesser.shape[5]
    tile = g.shape[5]
    copies = 7
    ticks = nz * points
    bunch = points // GROUPS
    e = lax.axis_index("energy")
    o = lax.axis_index("orb")
    c = lax.axis_index("kpt")
    ox = o + 1 - 2 * lax.rem(o, 2)
    oy = lax.rem(o + 2, 4)
    od = 3 - o
    cp = 1 - c
    to_x, to_y, to_peer = {"orb": ox}, {"orb": oy}, {"kpt": cp}

    def phase(i):
        return lax.div(i, points)

    def point(i):
        return lax.rem(i, points)

    def slot(i):
        return lax.rem(i, SLOTS)

    def offset(p):
        near = lax.div(p + 1, 2)
        return lax.select(lax.rem(p, 2) == 1, near, lax.rem(nz - lax.div(p, 2), nz))

    def owner(i):
        return lax.rem(e + nz - offset(phase(i)), nz)

    def rows(z):
        return pl.ds(pl.multiple_of(z * tile, tile), tile)

    def block(k, q, i):
        return g.at[k, q, point(i), owner(i)]

    def remote(src, dst, send_sem, recv_sem, target):
        return pltpu.make_async_remote_copy(
            src_ref=src,
            dst_ref=dst,
            send_sem=send_sem,
            recv_sem=recv_sem,
            device_id=target,
            device_id_type=MESH,
        )

    def z_start(n, _):
        p = lax.div(n, GROUPS) + 1
        some = pl.ds(lax.rem(n, GROUPS) * bunch, bunch)
        target = lax.rem(e + offset(p), nz)
        for part in range(2):
            remote(
                lesser.at[part, 0, some, 0, rows(target), :],
                g.at[c, o, some, e, part],
                zsend,
                zrecv.at[n],
                {"energy": target},
            ).start()
        return 0

    def z_arrival(n):
        ref = g.at[c, o, pl.ds(0, bunch), 0]
        return remote(ref, ref, zsend, zrecv.at[n], to_x)

    def z_sent():
        ref = g.at[c, pl.ds(0, nz - 1), :, 0]
        return remote(ref, ref, zsend, zrecv.at[0], to_x)

    pieces = (pl.ds(0, FIRST), pl.ds(FIRST, points - FIRST))

    def local_start(n):
        for part in range(2):
            pltpu.make_async_copy(
                lesser.at[part, 0, pieces[n], 0, rows(e), :],
                g.at[c, o, pieces[n], e, part],
                local_sem.at[n],
            ).start()

    def local_wait(n):
        ref = g.at[c, o, pieces[n], e]
        pltpu.make_async_copy(ref, ref, local_sem.at[n]).wait()

    def own_start(i):
        ref = block(c, o, i)
        for target in (to_x, to_y):
            remote(ref, ref, sent, orecv.at[slot(i)], target).start()

    def own_both(i):
        ref = g.at[c, pl.ds(0, 2), point(i), owner(i)]
        return remote(ref, ref, sent, orecv.at[slot(i)], to_x)

    def relay_start(i):
        for part, q, target in ((0, ox, to_y), (1, oy, to_x)):
            ref = g.at[c, q, point(i), owner(i), part]
            remote(ref, ref, sent, frecv.at[slot(i)], target).start()

    def relay_both(i):
        ref = block(c, od, i)
        return remote(ref, ref, sent, frecv.at[slot(i)], to_x)

    def all_sent():
        ref = g.at[:, :, :, :, :, pl.ds(0, tile * copies // 8), :]
        return remote(ref, ref, sent, orecv.at[0], to_x)

    def peer_sem(i, recv):
        return recv.at[lax.rem(i, recv.shape[0])]

    def peer_start(i, q, recv):
        ref = block(c, q, i)
        remote(ref, ref, sent, peer_sem(i, recv), to_peer).start()

    def peer_some(i, count, recv):
        ref = g.at[cp, pl.ds(0, count), point(i), owner(i)]
        return remote(ref, ref, sent, peer_sem(i, recv), to_peer)

    barrier = pltpu.get_barrier_semaphore()
    has_low, has_high = e > 0, e < nz - 1
    for target in (to_x, to_y, to_peer):
        pl.semaphore_signal(barrier, inc=1, device_id=target, device_id_type=MESH)

    def signal(sem, target, wanted):
        @pl.when(wanted)
        def _():
            pl.semaphore_signal(sem, inc=1, device_id={"energy": target}, device_id_type=MESH)

    signal(barrier, e - 1, has_low)
    signal(barrier, e + 1, has_high)
    for n in range(2):
        local_start(n)
    map_copy = pltpu.make_async_copy(map_hbm, map_ref, map_sem)
    map_copy.start()
    u_copy = pltpu.make_async_copy(coupling, u, u_sem)
    u_copy.start()
    acc[...] = jnp.zeros(acc.shape, acc.dtype)
    pl.semaphore_wait(barrier, 3 + has_low.astype(jnp.int32) + has_high.astype(jnp.int32))

    local_wait(0)
    for i in range(LEAD):
        if i == FIRST:
            local_wait(1)
        own_start(i)
        peer_start(i, o, precv)

    for h in range(nz - 2):
        signal(far.at[0, h], e - 1, has_low & (e + h + 1 < nz))
        signal(far.at[1, h], e + 1, has_high & (e - h - 1 >= 0))

        @pl.when(e + h + 2 < nz)
        def _(h=h):
            pl.semaphore_wait(far.at[0, h], 1)

        @pl.when(e - h - 2 >= 0)
        def _(h=h):
            pl.semaphore_wait(far.at[1, h], 1)

    lax.fori_loop(0, GROUPS, z_start, 0)
    map_copy.wait()
    u_copy.wait()

    def multiply(chunks, i, store):
        s = point(i)
        z = owner(i)
        half = lax.rem(phase(i), 2)

        def one(t, _):
            lhs, rhs = [], []
            for k, q in chunks:
                lhs.append(g[k, q, s, z, 0])
                lhs.append(g[k, q, s, z, 1])
                index = map_ref[c * points + t, k * points + s]
                at = pl.ds(pl.multiple_of(q * width, width), width)
                ur = u[0, index, at, :]
                ui = u[1, index, at, :]
                rhs.append(jnp.concatenate([ur, ui], axis=1))
                rhs.append(jnp.concatenate([-ui, ur], axis=1))
            product = jnp.dot(
                jnp.concatenate(lhs, axis=1),
                jnp.concatenate(rhs, axis=0),
                preferred_element_type=jnp.float32,
            )
            store(half, z, t, acc[half, t] + product)
            return 0

        lax.fori_loop(0, points, one, 0, unroll=True)

    def add(half, z, t, values):
        acc[half, t] = values

    def write(half, z, t, values):
        for part in range(2):
            out[part, z, t, 0] = values[:, part * width : (part + 1) * width].astype(out.dtype)

    near_chunks = ((c, o), (cp, o), (c, ox), (cp, ox), (c, oy), (cp, oy))
    far_chunks = ((c, od), (cp, od))

    def relay(r):
        own_both(r).wait_recv()
        relay_start(r)
        peer_start(r, ox, precv)
        peer_start(r, oy, precv)

    def diagonal(r):
        relay_both(r).wait_recv()
        peer_start(r, od, qrecv)

    def early(r):
        peer_some(r, 3, precv).wait_recv()
        multiply(near_chunks, r, add)

    def late(r):
        peer_some(r, 1, qrecv).wait_recv()
        multiply(far_chunks, r, add)

        @pl.when(point(r) == points - 1)
        def _():
            half = lax.rem(phase(r), 2)

            def flush(t, _):
                write(half, owner(r), t, acc[half, t])
                acc[half, t] = jnp.zeros(acc.shape[2:], acc.dtype)
                return 0

            lax.fori_loop(0, points, flush, 0, unroll=True)

    def after(i, bound):
        return (i >= bound).astype(jnp.int32)

    def tick(i, _):
        def stage(done, work):
            def one(r, _):
                work(r)
                return 0

            lax.fori_loop(done(i), done(i + 1), one, 0)

        @pl.when((i > 0) & (i <= (nz - 2) * PACE) & (lax.rem(i, PACE) == 0))
        def _():
            n = lax.div(i, PACE) * GROUPS
            lax.fori_loop(n, n + GROUPS, z_start, 0)

        def own(j):
            @pl.when((j >= points) & (lax.rem(j, bunch) == 0))
            def _():
                z_arrival(lax.div(j - points, bunch)).wait_recv()

            own_start(j)
            peer_start(j, o, precv)

        def own_done(j):
            return lax.max(lax.min(j + sum(after(j, a) for a in ADVANCE), ticks), LEAD)

        stage(own_done, own)

        def lagged(lag):
            return lambda j: lax.max(j - lag(j), 0)

        stage(lagged(lambda j: RELAY), relay)
        stage(lagged(lambda j: DIAG + after(j, DEEPER)), diagonal)
        stage(lagged(lambda j: EARLY + 1 - after(j, CATCH_UP)), early)
        stage(lagged(lambda j: LATE + after(j, DEEPER)), late)
        return 0

    lax.fori_loop(0, ticks - 1, tick, 0)
    last = ticks - 1
    relay(last - 2)
    early(last - 3)
    late(last - 7)
    diagonal(last - 6)
    relay(last - 1)
    early(last - 2)
    late(last - 6)
    diagonal(last - 5)
    relay(last)
    early(last - 1)
    diagonal(last - 4)
    late(last - 5)
    diagonal(last - 3)
    early(last)
    diagonal(last - 2)
    late(last - 4)
    diagonal(last - 1)
    late(last - 3)
    diagonal(last)
    late(last - 2)
    late(last - 1)
    multiply(far_chunks[:1], last, add)
    peer_some(last, 1, qrecv).wait_recv()
    multiply(far_chunks[1:], last, write)
    all_sent().wait_send()
    z_sent().wait_send()


def per_device_fused(nz, lesser, coupling, transfer_map):
    points = lesser.shape[2]
    tile = lesser.shape[4] // nz
    width = lesser.shape[5]
    out_cols = coupling.shape[3]
    dma = pltpu.SemaphoreType.DMA
    lesser, coupling, transfer_map = (
        pltpu.with_memory_space_constraint(x, pltpu.HBM) for x in (lesser, coupling, transfer_map)
    )
    return pl.pallas_call(
        functools.partial(kernel, nz),
        out_shape=jax.ShapeDtypeStruct((2, nz, points, 1, tile, out_cols), jnp.bfloat16),
        in_specs=[pl.BlockSpec(memory_space=pltpu.HBM)] * 3,
        out_specs=pl.BlockSpec(memory_space=pltpu.VMEM),
        scratch_shapes=[
            pltpu.VMEM((2, 4, points, nz, 2, tile, width), lesser.dtype),
            pltpu.VMEM(coupling.shape, coupling.dtype),
            pltpu.VMEM((2, points, tile, 2 * out_cols), jnp.float32),
            pltpu.SMEM(transfer_map.shape, transfer_map.dtype),
            dma((3, SLOTS)),
            dma((DIAG_SLOTS,)),
            dma(()),
            dma(()),
            dma(((nz - 1) * GROUPS,)),
            pltpu.SemaphoreType.REGULAR((2, max(nz - 2, 1))),
            dma((2,)),
            dma(()),
            dma(()),
        ],
        compiler_params=pltpu.CompilerParams(
            collective_id=0, has_side_effects=True, vmem_limit_bytes=40 * 1024 * 1024
        ),
    )(transfer_map, lesser, coupling)


def solution(mesh):
    in_specs = (P(None, "energy", "kpt", None, None, "orb"), P(None, None, None, "orb"), P())
    out_specs = P(None, None, "kpt", None, "energy", "orb")
    nz = mesh.shape["energy"]

    def per_device(lesser, coupling, transfer_map):
        shape = lesser.shape
        fused = (
            mesh.shape["orb"] == 4
            and mesh.shape["kpt"] == 2
            and nz > 1
            and shape[1] == 1
            and shape[3] == 1
            and shape[5] == coupling.shape[3] == 128
            and shape[4] == nz * 128
            and shape[2] % GROUPS == 0
            and shape[2] % 2 == 0
            and shape[2] >= max(LEAD, PACE)
            and nz * shape[2] > max(CATCH_UP, DEEPER, LATE, *ADVANCE)
        )
        if fused:
            return per_device_fused(nz, lesser, coupling, transfer_map)
        return per_device_general(lesser, coupling, transfer_map)

    return jax.shard_map(
        per_device, mesh=mesh, in_specs=in_specs, out_specs=out_specs, check_vma=False
    )
```
